32 devices in a mesh: section: 4 (over y, x), dp: 8 (over z, core).
Axes of the slice: x: 2, y: 2, z: 4, core: 2. Of those that a mesh axis runs over, the one named last changes fastest.
Arguments:
- grads: float32 [4, 8, 64, 4096], P('section', 'dp'), may hold values from -4096 to 4096
- skipped: int32 [8], P('dp'), may hold values from 0 to 24
- master: float32 [4, 64, 4096], P('section', 'dp'), may hold values from -6 to 6
- moment_one: float32 [4, 64, 4096], P('section', 'dp'), may hold values from -6 to 6
- moment_two: float32 [4, 64, 4096], P('section', 'dp'), may hold values from 0.25 to 4
- bounds: int32 [4, 9], P('section'), may hold values from 0 to 64, as said below
- step: int32 [1], replicated, may hold values from 1 to 24
Outputs:
- params: bfloat16 [4, 64, 4096], P('section')
- master_next: float32 [4, 64, 4096], P('section', 'dp')
- moment_one_next: float32 [4, 64, 4096], P('section', 'dp')
- moment_two_next: float32 [4, 64, 4096], P('section', 'dp')
- layer_norms: float32 [4, 8], P('section')
- grad_norm: float32 [1], replicated
The draws below stay inside these ranges and needn't reach their ends.
Inputs may be any that keep to these rules, and one draw needn't show every extreme that they name: `bounds`: each section's row is strictly increasing, starts at 0 and ends at 64.
All inputs are finite; a program needn't handle non-finite values.
Results may differ from the reference program's by a relative error of at most 0.001.
Values may be sent and summed in bfloat16 or wider, within the bound.
A program may use at most 64 MiB of HBM per device.

```python
import math
import jax
import jax.numpy as jnp
from jax import lax

D = 4096
LAYERS = 8
MICRO = 32
ROWS = 64
N_SECTION = 4
N_DP = 8


def section_bounds(key):
    inner = jax.random.permutation(key, ROWS - 1)[:LAYERS - 1] + 1
    inner = jnp.sort(inner.astype(jnp.int32))
    return jnp.concatenate([jnp.zeros((1,), jnp.int32), inner, jnp.full((1,), ROWS, jnp.int32)])


def draw_bounds(key, part):
    return jnp.stack([section_bounds(jax.random.fold_in(key, 7 + index)) for index in range(N_SECTION)])


def set_ends(drawn, stream_key, least, high):
    extent = drawn.shape
    spot = [jax.random.randint(jax.random.fold_in(stream_key, axis), (), 0, extent[axis]) for axis in range(len(extent))]
    drawn = drawn.at[tuple(spot)].set(least)
    longest = extent.index(max(extent))
    spot[longest] = (spot[longest] + 1) % extent[longest]
    return drawn.at[tuple(spot)].set(high)


def with_spikes(array, own_key, source, target, shards_of, factor):
    owner, partner = [(jnp.arange(array.shape[dim]) // (array.shape[dim] // shards_of)).reshape([-1 if axis == dim else 1 for axis in range(array.ndim)]) for dim in (source, target)]
    chosen = jax.random.permutation(own_key, shards_of)[partner]
    strong = (owner == chosen) | (owner == (partner + shards_of // 2) % shards_of)
    return jnp.where(strong, factor * array, array)


def shard_levels(key, shape, pieces, low, top_value):
    gain = 1.0
    for axis_at, blocks in pieces:
        heights = jax.random.uniform(jax.random.fold_in(jax.random.fold_in(key, 6), axis_at), (blocks,), jnp.float32, low / len(pieces), top_value / len(pieces))
        gain = gain * jnp.repeat(jnp.exp(heights), shape[axis_at] // blocks).reshape((-1,) + (1,) * (len(shape) - 1 - axis_at))
    return gain


def noise(rng, dims, width, bound, pieces=(), kind=jnp.bfloat16):
    drawn = jax.random.normal(rng, dims, jnp.float32) * width
    if len(pieces) > 0:
        drawn = shard_levels(rng, dims, pieces, -0.22, 0.18) * drawn
    return jnp.clip(drawn, min=-bound, max=bound).astype(kind)


def heavy_noise(rng, shape, scale, limit, cuts, heavy, held_as=jnp.bfloat16):
    values = scale * jax.random.normal(rng, shape, jnp.float32)
    if cuts:
        values = values * shard_levels(rng, shape, cuts, -0.22, 0.18)
    return jnp.clip(with_spikes(values, jax.random.fold_in(rng, 3), *heavy), -limit, limit).astype(held_as)


def setup_inputs(seed: int = 0) -> dict:
    seeds = jax.random.split(jax.random.key(seed), 8)
    return {
        "grads": heavy_noise(seeds[0], (N_SECTION, N_DP, ROWS, D), 500.0, 4096.0, ((0, 4), (1, 8)), (1, 2, 8, 2.0), jnp.float32),
        "skipped": set_ends(jax.random.randint(seeds[1], (N_DP,), 0, 25), jax.random.fold_in(seeds[1], 1), 0, 24).astype(jnp.int32),
        "master": noise(seeds[2], (N_SECTION, ROWS, D), 1.0, 6.0, ((0, 4), (1, 8)), jnp.float32),
        "moment_one": noise(seeds[3], (N_SECTION, ROWS, D), 1.0, 6.0, ((0, 4), (1, 8)), jnp.float32),
        "moment_two": jnp.clip(jnp.exp(math.log(4.0) - 2.7725887 * jax.random.uniform(seeds[4], (N_SECTION, ROWS, D), jnp.float32) ** shard_levels(seeds[4], (N_SECTION, ROWS, D), ((0, 4), (1, 8)), -0.2, 0.2)), 0.25, 4.0),
        "bounds": draw_bounds(jax.random.fold_in(seeds[7], 71), 0),
        "step": jax.random.randint(seeds[6], (1,), 1, 25).astype(jnp.int32),
    }


beta_one = 0.9
beta_two = 0.95
learn_rate = 0.05
weight_decay = 0.1
epsilon = 1e-08

def reference(grads, skipped, master, moment_one, moment_two, bounds, step):
    total_good = jnp.sum((MICRO - skipped).astype(jnp.float32))
    summed = lax.optimization_barrier(jnp.sum(grads, axis=1))
    mean_grad = summed / total_good
    row_squares = lax.optimization_barrier(jnp.sum(mean_grad * mean_grad, axis=2))
    row_index = jnp.arange(ROWS, dtype=jnp.int32)
    inside = (row_index[None, :, None] >= bounds[:, None, :-1]) & (row_index[None, :, None] < bounds[:, None, 1:])
    layer_sq = lax.optimization_barrier(jnp.sum(row_squares[:, :, None] * inside.astype(jnp.float32), axis=1))
    grad_rms = jnp.sqrt(jnp.sum(layer_sq) / (N_SECTION * ROWS * D))
    layer_rows = (bounds[:, 1:] - bounds[:, :-1]).astype(jnp.float32)
    layer_norms = jnp.sqrt(layer_sq / (layer_rows * D))
    clipped = mean_grad / jnp.maximum(1.0, grad_rms)
    first_next = beta_one * moment_one + (1.0 - beta_one) * clipped
    second_next = beta_two * moment_two + (1.0 - beta_two) * clipped * clipped
    step_value = step[0].astype(jnp.float32)
    fix_one = 1.0 - jnp.power(beta_one, step_value)
    fix_two = 1.0 - jnp.power(beta_two, step_value)
    update = first_next / fix_one / (jnp.sqrt(second_next / fix_two) + epsilon)
    master_next = master - learn_rate * (update + weight_decay * master)
    params = master_next.astype(jnp.bfloat16)
    return (params, master_next, first_next, second_next, layer_norms, grad_rms.reshape(1))
```

```python
import functools
import math

import jax
import jax.numpy as jnp
from jax import lax
from jax.experimental import pallas as pl
from jax.experimental.pallas import tpu as pltpu
from jax.sharding import PartitionSpec as P

MICRO = 32
PAIR = 2

beta_one = 0.9
beta_two = 0.95
learn_rate = 0.05
weight_decay = 0.1
epsilon = 1e-08

MESH = pl.DeviceIdType.MESH
LANES = 128


def repeat(count, body):
    if count <= 8:
        for index in range(count):
            body(index)
    else:
        lax.fori_loop(0, count, lambda index, _: (body(index), None)[1], None)


def kernel(
    n_section,
    n_dp,
    layers,
    grads,
    skipped,
    master,
    moment_one,
    moment_two,
    bounds,
    step,
    params,
    master_next,
    first_next,
    second_next,
    layer_norms,
    grad_norm,
    mine,
    theirs,
    paired,
    outgoing,
    incoming,
    dp_stats,
    section_stats,
    state,
    result,
    load_sem,
    pair_send,
    pair_recv,
    sum_send,
    sum_recv,
    stat_send,
    stat_recv,
    sec_send,
    sec_recv,
    row_send,
    row_recv,
    near_send,
    near_recv,
    store_sem,
):
    section = lax.axis_index("section")
    me = lax.axis_index("dp")
    n_chip = n_dp // PAIR
    chip, core = me // PAIR, lax.rem(me, PAIR)
    other = 1 - core
    partner = chip * PAIR + other
    own_rows, width = mine.shape[1], mine.shape[2]
    rows_all = n_dp * own_rows

    def remote(src, dst, send, recv, sec, dp):
        return pltpu.make_async_remote_copy(
            src_ref=src, dst_ref=dst, send_sem=send, recv_sem=recv,
            device_id=(sec, dp), device_id_type=MESH,
        )

    load_theirs = pltpu.make_async_copy(grads.at[:, other], theirs, load_sem.at[0])
    load_mine = pltpu.make_async_copy(grads.at[:, core], mine, load_sem.at[1])
    load_theirs.start()
    load_mine.start()
    state_loads = [
        pltpu.make_async_copy(source, state.at[k], load_sem.at[2 + k])
        for k, source in enumerate((master, moment_one, moment_two))
    ]
    for load in state_loads:
        load.start()

    barrier = pltpu.get_barrier_semaphore()

    def greet_dp(k):
        pl.semaphore_signal(
            barrier, inc=1, device_id=(section, lax.rem(me + k + 1, n_dp)), device_id_type=MESH
        )

    def greet_section(k):
        pl.semaphore_signal(
            barrier, inc=1, device_id=(lax.rem(section + k + 1, n_section), me), device_id_type=MESH
        )

    repeat(n_dp - 1, greet_dp)
    repeat(n_section - 1, greet_section)
    pl.semaphore_wait(barrier, n_dp + n_section - 2)

    def pair_copy(off):
        z = lax.rem(chip + off, n_chip)
        return remote(
            theirs.at[z], paired.at[z], pair_send.at[off], pair_recv.at[off], section, partner
        )

    def order(k):
        return k + 1 if isinstance(k, int) and k + 1 < n_chip else lax.rem(k + 1, n_chip)

    load_theirs.wait()
    repeat(n_chip, lambda k: pair_copy(order(k)).start())
    load_mine.wait()

    def sum_copy(k):
        z = lax.rem(chip + k + 1, n_chip)
        return remote(
            outgoing.at[k], incoming.at[k], sum_send.at[k], sum_recv.at[k], section, z * PAIR + core
        )

    def send_sum(k):
        z = lax.rem(chip + k + 1, n_chip)
        pair_copy(k + 1).wait_recv()
        outgoing[k] = (mine[z] + paired[z]).astype(jnp.bfloat16)
        sum_copy(k).start()

    repeat(n_chip - 1, send_sum)
    pair_copy(0).wait_recv()
    mine[chip] = mine[chip] + paired[chip]

    def take_sum(k):
        sum_copy(k).wait_recv()
        mine[chip] = mine[chip] + incoming[k].astype(jnp.float32)

    repeat(n_chip - 1, take_sum)
    total_grad = mine[chip]

    row_squares = jnp.sum(total_grad * total_grad, axis=1, keepdims=True)
    row = me * own_rows + lax.broadcasted_iota(jnp.int32, (own_rows, LANES), 0)
    lane = lax.broadcasted_iota(jnp.int32, (1, LANES), 1)
    low = jnp.zeros((1, LANES), jnp.int32)
    high = jnp.zeros((1, LANES), jnp.int32)
    for layer in range(layers):
        low = jnp.where(lane == layer, bounds[0, layer], low)
        high = jnp.where(lane == layer, bounds[0, layer + 1], high)
    inside = (row >= low) & (row < high)
    own_stats = jnp.sum(jnp.where(inside, row_squares, 0.0), axis=0, keepdims=True)
    good = (MICRO - skipped[0]).astype(jnp.float32)
    dp_stats[me] = jnp.where(lane == layers, good, own_stats)

    def stat_copy(k):
        return remote(
            dp_stats.at[me], dp_stats.at[me], stat_send.at[k], stat_recv.at[k],
            section, lax.rem(me + k + 1, n_dp),
        )

    repeat(n_dp - 1, lambda k: stat_copy(k).start())
    for load in state_loads:
        load.wait()
    step_value = jnp.full((1, 1), step[0], jnp.int32).astype(jnp.float32)
    fix_one = 1.0 - jnp.exp(step_value * math.log(beta_one))
    fix_two = 1.0 - jnp.exp(step_value * math.log(beta_two))
    repeat(n_dp - 1, lambda k: stat_copy(k).wait_recv())
    section_sum = jnp.sum(dp_stats[...], axis=0)
    section_stats[section] = section_sum

    def section_copy(k):
        return remote(
            section_stats.at[section], section_stats.at[section], sec_send.at[k], sec_recv.at[k],
            lax.rem(section + k + 1, n_section), me,
        )

    repeat(n_section - 1, lambda k: section_copy(k).start())
    total_good = jnp.sum(jnp.where(lane == layers, section_sum, 0.0), axis=1, keepdims=True)
    layer_rows = jnp.where(lane < layers, high - low, 1).astype(jnp.float32)
    norms = jnp.sqrt(section_sum / (layer_rows * width)) / total_good
    layer_norms[...] = norms[:, :layers]
    repeat(n_section - 1, lambda k: section_copy(k).wait_recv())
    everything = jnp.sum(section_stats[...], axis=0)
    total_sq = jnp.sum(jnp.where(lane < layers, everything, 0.0), axis=1, keepdims=True)
    grad_rms = jnp.sqrt(total_sq / (n_section * rows_all * width)) / total_good
    grad_norm[...] = grad_rms

    clipped = total_grad * (1.0 / (total_good * jnp.maximum(1.0, grad_rms)))
    one = beta_one * state[1] + (1.0 - beta_one) * clipped
    two = beta_two * state[2] + (1.0 - beta_two) * clipped * clipped
    update = one * (1.0 / fix_one) / (jnp.sqrt(two * (1.0 / fix_two)) + epsilon)
    master_new = state[0] - learn_rate * (update + weight_decay * state[0])
    params[me] = master_new.astype(jnp.bfloat16)

    def near_copy(off):
        block = lax.rem(chip + off, n_chip) * PAIR + core
        return remote(
            params.at[block], params.at[block], near_send.at[off], near_recv.at[off], section, partner
        )

    def row_copy(k):
        return remote(
            params.at[me], params.at[me], row_send.at[k], row_recv.at[k],
            section, lax.rem(chip + k + 1, n_chip) * PAIR + core,
        )

    repeat(n_chip - 1, lambda k: row_copy(k).start())
    near_copy(0).start()
    result[0] = master_new
    result[1] = one
    result[2] = two
    stores = [
        pltpu.make_async_copy(result.at[k], target, store_sem.at[k])
        for k, target in enumerate((master_next, first_next, second_next))
    ]
    for store in stores:
        store.start()

    def pass_on(k):
        row_copy(k).wait_recv()
        near_copy(n_chip - 1 - k).start()

    repeat(n_chip - 1, pass_on)
    repeat(n_chip, lambda k: near_copy(k).wait_recv())
    for store in stores:
        store.wait()
    repeat(n_chip, lambda k: pair_copy(k).wait_send())
    repeat(n_chip - 1, lambda k: sum_copy(k).wait_send())
    repeat(n_dp - 1, lambda k: stat_copy(k).wait_send())
    repeat(n_section - 1, lambda k: section_copy(k).wait_send())
    repeat(n_chip - 1, lambda k: row_copy(k).wait_send())
    repeat(n_chip, lambda k: near_copy(k).wait_send())


def on_device(n_section, n_dp, grads, skipped, master, moment_one, moment_two, bounds, step):
    rows_all, width = grads.shape[2:]
    own_rows = master.shape[1]
    layers = bounds.shape[1] - 1
    n_chip = n_dp // PAIR
    any_space = pl.BlockSpec(memory_space=pl.ANY)
    smem = pl.BlockSpec(memory_space=pltpu.SMEM)
    vmem = pl.BlockSpec(memory_space=pltpu.VMEM)
    own = jax.ShapeDtypeStruct((own_rows, width), jnp.float32)
    dma = pltpu.SemaphoreType.DMA
    blocks = pltpu.VMEM((n_chip, own_rows, width), jnp.float32)
    halves = pltpu.VMEM((n_chip - 1, own_rows, width), jnp.bfloat16)
    params, master_next, first_next, second_next, layer_norms, grad_norm = pl.pallas_call(
        functools.partial(kernel, n_section, n_dp, layers),
        out_shape=(
            jax.ShapeDtypeStruct((n_dp, own_rows, width), jnp.bfloat16),
            own,
            own,
            own,
            jax.ShapeDtypeStruct((1, layers), jnp.float32),
            jax.ShapeDtypeStruct((1, 1), jnp.float32),
        ),
        in_specs=[any_space, smem, any_space, any_space, any_space, smem, smem],
        out_specs=(vmem, any_space, any_space, any_space, vmem, vmem),
        scratch_shapes=[
            blocks,
            blocks,
            blocks,
            halves,
            halves,
            pltpu.VMEM((n_dp, 1, LANES), jnp.float32),
            pltpu.VMEM((n_section, 1, LANES), jnp.float32),
            pltpu.VMEM((3, own_rows, width), jnp.float32),
            pltpu.VMEM((3, own_rows, width), jnp.float32),
            dma((5,)),
            dma((n_chip,)),
            dma((n_chip,)),
            dma((n_chip - 1,)),
            dma((n_chip - 1,)),
            dma((n_dp - 1,)),
            dma((n_dp - 1,)),
            dma((n_section - 1,)),
            dma((n_section - 1,)),
            dma((n_chip - 1,)),
            dma((n_chip - 1,)),
            dma((n_chip,)),
            dma((n_chip,)),
            dma((3,)),
        ],
        compiler_params=pltpu.CompilerParams(collective_id=0, has_side_effects=True),
    )(
        grads.reshape(n_chip, PAIR, own_rows, width),
        skipped,
        master[0],
        moment_one[0],
        moment_two[0],
        bounds,
        step,
    )
    return (
        params.reshape(1, rows_all, width),
        master_next[None],
        first_next[None],
        second_next[None],
        layer_norms,
        grad_norm.reshape(1),
    )


def solution(mesh):
    in_specs = (
        P("section", "dp", None, None),
        P("dp"),
        P("section", "dp", None),
        P("section", "dp", None),
        P("section", "dp", None),
        P("section", None),
        P(),
    )
    out_specs = (
        P("section", None, None),
        P("section", "dp", None),
        P("section", "dp", None),
        P("section", "dp", None),
        P("section", None),
        P(),
    )
    body = functools.partial(on_device, mesh.shape["section"], mesh.shape["dp"])
    return jax.shard_map(
        body, mesh=mesh, in_specs=in_specs, out_specs=out_specs, check_vma=False
    )
```

```python
import functools
import math

import jax
import jax.numpy as jnp
from jax import lax
from jax.experimental import pallas as pl
from jax.experimental.pallas import tpu as pltpu
from jax.sharding import PartitionSpec as P

MICRO = 32
PAIR = 2

beta_one = 0.9
beta_two = 0.95
learn_rate = 0.05
weight_decay = 0.1
epsilon = 1e-08

MESH = pl.DeviceIdType.MESH
LANES = 128
SLACK = 2**20
SPARE = 2**14
VMEM_BYTES = 67043328


def repeat(count, body):
    if count <= 8:
        for index in range(count):
            body(index)
    else:
        lax.fori_loop(0, count, lambda index, _: (body(index), None)[1], None)


def kernel(
    n_section,
    n_dp,
    layers,
    grads,
    counts,
    master,
    moment_one,
    moment_two,
    bounds,
    params,
    result,
    norms_out,
    mine,
    theirs,
    paired,
    outgoing,
    incoming,
    dp_stats,
    section_stats,
    state,
    counts_in,
    bounds_in,
    load_sem,
    pair_send,
    pair_recv,
    sum_send,
    sum_recv,
    stat_send,
    stat_recv,
    sec_send,
    sec_recv,
    row_send,
    row_recv,
    near_send,
    near_recv,
):
    section = lax.axis_index("section")
    me = lax.axis_index("dp")
    n_chip = n_dp // PAIR
    chip, core = me // PAIR, lax.rem(me, PAIR)
    other = 1 - core
    partner = chip * PAIR + other
    own_rows, width = mine.shape[1], mine.shape[2]
    rows_all = n_dp * own_rows

    def remote(src, dst, send, recv, sec, dp):
        return pltpu.make_async_remote_copy(
            src_ref=src, dst_ref=dst, send_sem=send, recv_sem=recv,
            device_id=(sec, dp), device_id_type=MESH,
        )

    barrier = pltpu.get_barrier_semaphore()

    def greet_dp(k):
        pl.semaphore_signal(
            barrier, inc=1, device_id=(section, lax.rem(me + k + 1, n_dp)), device_id_type=MESH
        )

    def greet_section(k):
        pl.semaphore_signal(
            barrier, inc=1, device_id=(lax.rem(section + k + 1, n_section), me), device_id_type=MESH
        )

    repeat(n_dp - 1, greet_dp)
    repeat(n_section - 1, greet_section)
    load_theirs = pltpu.make_async_copy(grads.at[:, other], theirs, load_sem.at[0])
    load_mine = pltpu.make_async_copy(grads.at[:, core], mine, load_sem.at[1])
    load_theirs.start()
    load_mine.start()
    state_loads = [
        pltpu.make_async_copy(source, state.at[k], load_sem.at[2 + k])
        for k, source in enumerate((master, moment_one, moment_two))
    ]
    state_loads += [
        pltpu.make_async_copy(source, target, load_sem.at[5 + k])
        for k, (source, target) in enumerate(
            ((counts, counts_in), (bounds, bounds_in))
        )
    ]
    for load in state_loads:
        load.start()

    pl.semaphore_wait(barrier, n_dp + n_section - 2)

    def pair_copy(off):
        z = lax.rem(chip + off, n_chip)
        return remote(
            theirs.at[z], paired.at[z], pair_send.at[off], pair_recv.at[off], section, partner
        )

    def order(k):
        return k + 1 if isinstance(k, int) and k + 1 < n_chip else lax.rem(k + 1, n_chip)

    load_theirs.wait()
    repeat(n_chip, lambda k: pair_copy(order(k)).start())
    load_mine.wait()

    def sum_copy(k):
        z = lax.rem(chip + k + 1, n_chip)
        return remote(
            outgoing.at[k], incoming.at[k], sum_send.at[k], sum_recv.at[k], section, z * PAIR + core
        )

    def send_sum(k):
        z = lax.rem(chip + k + 1, n_chip)
        pair_copy(k + 1).wait_recv()
        outgoing[k] = (mine[z] + paired[z]).astype(jnp.bfloat16)
        sum_copy(k).start()

    repeat(n_chip - 1, send_sum)
    pair_copy(0).wait_recv()
    mine[chip] = mine[chip] + paired[chip]

    def take_sum(k):
        sum_copy(k).wait_recv()
        mine[chip] = mine[chip] + incoming[k].astype(jnp.float32)

    repeat(n_chip - 1, take_sum)
    total_grad = mine[chip]

    for load in state_loads:
        load.wait()
    row_squares = jnp.sum(total_grad * total_grad, axis=1, keepdims=True)
    row = me * own_rows + lax.broadcasted_iota(jnp.int32, (own_rows, LANES), 0)
    lane = lax.broadcasted_iota(jnp.int32, (1, LANES), 1)
    low = jnp.zeros((1, LANES), jnp.int32)
    high = jnp.zeros((1, LANES), jnp.int32)
    for layer in range(layers):
        low = jnp.where(lane == layer, bounds_in[0, layer], low)
        high = jnp.where(lane == layer, bounds_in[0, layer + 1], high)
    inside = (row >= low) & (row < high)
    own_stats = jnp.sum(jnp.where(inside, row_squares, 0.0), axis=0, keepdims=True)
    good = (MICRO - counts_in[0, 0]).astype(jnp.float32)
    dp_stats[me] = jnp.where(lane == layers, good, own_stats)

    def stat_copy(k):
        return remote(
            dp_stats.at[me], dp_stats.at[me], stat_send.at[k], stat_recv.at[k],
            section, lax.rem(me + k + 1, n_dp),
        )

    repeat(n_dp - 1, lambda k: stat_copy(k).start())
    step_value = jnp.full((1, 1), counts_in[0, 1], jnp.int32).astype(jnp.float32)
    fix_one = 1.0 - jnp.exp(step_value * math.log(beta_one))
    fix_two = 1.0 - jnp.exp(step_value * math.log(beta_two))
    repeat(n_dp - 1, lambda k: stat_copy(k).wait_recv())
    section_sum = jnp.sum(dp_stats[...], axis=0)
    section_stats[section] = section_sum

    def section_copy(k):
        return remote(
            section_stats.at[section], section_stats.at[section], sec_send.at[k], sec_recv.at[k],
            lax.rem(section + k + 1, n_section), me,
        )

    repeat(n_section - 1, lambda k: section_copy(k).start())
    total_good = jnp.sum(jnp.where(lane == layers, section_sum, 0.0), axis=1, keepdims=True)
    layer_rows = jnp.where(lane < layers, high - low, 1).astype(jnp.float32)
    norms = jnp.sqrt(section_sum / (layer_rows * width)) / total_good
    norms_out[0] = norms
    repeat(n_section - 1, lambda k: section_copy(k).wait_recv())
    everything = jnp.sum(section_stats[...], axis=0)
    total_sq = jnp.sum(jnp.where(lane < layers, everything, 0.0), axis=1, keepdims=True)
    grad_rms = jnp.sqrt(total_sq / (n_section * rows_all * width)) / total_good
    norms_out[1] = jnp.broadcast_to(grad_rms, (1, LANES))

    clipped = total_grad * (1.0 / (total_good * jnp.maximum(1.0, grad_rms)))
    one = beta_one * state[1] + (1.0 - beta_one) * clipped
    two = beta_two * state[2] + (1.0 - beta_two) * clipped * clipped
    update = one * (1.0 / fix_one) / (jnp.sqrt(two * (1.0 / fix_two)) + epsilon)
    master_new = state[0] - learn_rate * (update + weight_decay * state[0])
    params[me] = master_new.astype(jnp.bfloat16)

    def near_copy(off):
        block = lax.rem(chip + off, n_chip) * PAIR + core
        return remote(
            params.at[block], params.at[block], near_send.at[off], near_recv.at[off], section, partner
        )

    def row_copy(k):
        return remote(
            params.at[me], params.at[me], row_send.at[k], row_recv.at[k],
            section, lax.rem(chip + k + 1, n_chip) * PAIR + core,
        )

    repeat(n_chip - 1, lambda k: row_copy(k).start())
    near_copy(0).start()
    result[0] = master_new
    result[1] = one
    result[2] = two

    def pass_on(k):
        row_copy(k).wait_recv()
        near_copy(n_chip - 1 - k).start()

    repeat(n_chip - 1, pass_on)
    repeat(n_chip, lambda k: near_copy(k).wait_recv())
    repeat(n_chip, lambda k: pair_copy(k).wait_send())
    repeat(n_chip - 1, lambda k: sum_copy(k).wait_send())
    repeat(n_dp - 1, lambda k: stat_copy(k).wait_send())
    repeat(n_section - 1, lambda k: section_copy(k).wait_send())
    repeat(n_chip - 1, lambda k: row_copy(k).wait_send())
    repeat(n_chip, lambda k: near_copy(k).wait_send())


def write_out(params, result, norms, params_out, master_next, first_next, second_next, layer_norms, grad_norm, sem):
    copies = [pltpu.make_async_copy(params, params_out, sem.at[3])]
    copies += [
        pltpu.make_async_copy(result.at[k], target, sem.at[k])
        for k, target in enumerate((master_next, first_next, second_next))
    ]
    for copy in copies:
        copy.start()
    layer_norms[...] = norms[0][:, : layer_norms.shape[1]]
    grad_norm[...] = norms[1][:, :1]
    for copy in copies:
        copy.wait()


def on_device(n_section, n_dp, grads, skipped, master, moment_one, moment_two, bounds, step):
    rows_all, width = grads.shape[2:]
    own_rows = master.shape[1]
    layers = bounds.shape[1] - 1
    n_chip = n_dp // PAIR
    hbm = pl.BlockSpec(memory_space=pltpu.HBM)
    held_bytes = rows_all * width * 2 + 3 * own_rows * width * 4 + SPARE
    vmem = pl.BlockSpec(memory_space=pltpu.VMEM)
    own = jax.ShapeDtypeStruct((own_rows, width), jnp.float32)
    dma = pltpu.SemaphoreType.DMA
    blocks = pltpu.VMEM((n_chip, own_rows, width), jnp.float32)
    halves = pltpu.VMEM((n_chip - 1, own_rows, width), jnp.bfloat16)
    held = pl.pallas_call(
        functools.partial(kernel, n_section, n_dp, layers),
        out_shape=(
            pltpu.VMEM((n_dp, own_rows, width), jnp.bfloat16),
            pltpu.VMEM((3, own_rows, width), jnp.float32),
            pltpu.VMEM((2, 1, LANES), jnp.float32),
        ),
        in_specs=[hbm] * 6,
        out_specs=(vmem, vmem, vmem),
        scratch_shapes=[
            blocks,
            blocks,
            blocks,
            halves,
            halves,
            pltpu.VMEM((n_dp, 1, LANES), jnp.float32),
            pltpu.VMEM((n_section, 1, LANES), jnp.float32),
            pltpu.VMEM((3, own_rows, width), jnp.float32),
            pltpu.SMEM((1, 2), jnp.int32),
            pltpu.SMEM(bounds.shape, jnp.int32),
            dma((7,)),
            dma((n_chip,)),
            dma((n_chip,)),
            dma((n_chip - 1,)),
            dma((n_chip - 1,)),
            dma((n_dp - 1,)),
            dma((n_dp - 1,)),
            dma((n_section - 1,)),
            dma((n_section - 1,)),
            dma((n_chip - 1,)),
            dma((n_chip - 1,)),
            dma((n_chip,)),
            dma((n_chip,)),
        ],
        compiler_params=pltpu.CompilerParams(
            collective_id=0, has_side_effects=True, vmem_limit_bytes=VMEM_BYTES - held_bytes
        ),
    )(
        grads.reshape(n_chip, PAIR, own_rows, width),
        jnp.concatenate((skipped, step))[None],
        master[0],
        moment_one[0],
        moment_two[0],
        bounds,
    )
    params, master_next, first_next, second_next, layer_norms, grad_norm = pl.pallas_call(
        write_out,
        out_shape=(
            jax.ShapeDtypeStruct((n_dp, own_rows, width), jnp.bfloat16),
            own,
            own,
            own,
            jax.ShapeDtypeStruct((1, layers), jnp.float32),
            jax.ShapeDtypeStruct((1, 1), jnp.float32),
        ),
        in_specs=[vmem] * 3,
        out_specs=(hbm, hbm, hbm, hbm, vmem, vmem),
        scratch_shapes=[dma((4,))],
        compiler_params=pltpu.CompilerParams(vmem_limit_bytes=SLACK),
    )(*held)
    return (
        params.reshape(1, rows_all, width),
        master_next[None],
        first_next[None],
        second_next[None],
        layer_norms,
        grad_norm.reshape(1),
    )


def solution(mesh):
    in_specs = (
        P("section", "dp", None, None),
        P("dp"),
        P("section", "dp", None),
        P("section", "dp", None),
        P("section", "dp", None),
        P("section", None),
        P(),
    )
    out_specs = (
        P("section", None, None),
        P("section", "dp", None),
        P("section", "dp", None),
        P("section", "dp", None),
        P("section", None),
        P(),
    )
    body = functools.partial(on_device, mesh.shape["section"], mesh.shape["dp"])
    return jax.shard_map(
        body, mesh=mesh, in_specs=in_specs, out_specs=out_specs, check_vma=False
    )
```

```python
import functools
import math

import jax
import jax.numpy as jnp
from jax import lax
from jax.experimental import pallas as pl
from jax.experimental.pallas import tpu as pltpu
from jax.sharding import PartitionSpec as P

MICRO = 32
PAIR = 2

beta_one = 0.9
beta_two = 0.95
learn_rate = 0.05
weight_decay = 0.1
epsilon = 1e-08

MESH = pl.DeviceIdType.MESH
LANES = 128
SLACK = 2**20
SPARE = 2**14
VMEM_BYTES = 67043328


def repeat(count, body):
    if count <= 8:
        for index in range(count):
            body(index)
    else:
        lax.fori_loop(0, count, lambda index, _: (body(index), None)[1], None)


def kernel(
    n_section,
    n_dp,
    layers,
    grads,
    skipped,
    master,
    moment_one,
    moment_two,
    bounds,
    step,
    params,
    result,
    norms_out,
    mine,
    theirs,
    paired,
    outgoing,
    incoming,
    stats,
    state,
    bounds_in,
    load_sem,
    pair_send,
    pair_recv,
    sum_send,
    sum_recv,
    stat_send,
    stat_recv,
    row_send,
    row_recv,
    near_send,
    near_recv,
):
    section = lax.axis_index("section")
    me = lax.axis_index("dp")
    n_chip = n_dp // PAIR
    chip, core = me // PAIR, lax.rem(me, PAIR)
    other = 1 - core
    partner = chip * PAIR + other
    own_rows, width = mine.shape[1], mine.shape[2]
    rows_all = n_dp * own_rows
    place = section * n_dp + me

    def remote(src, dst, send, recv, sec, dp):
        return pltpu.make_async_remote_copy(
            src_ref=src, dst_ref=dst, send_sem=send, recv_sem=recv,
            device_id=(sec, dp), device_id_type=MESH,
        )

    barrier = pltpu.get_barrier_semaphore()

    def greet_dp(k):
        pl.semaphore_signal(
            barrier, inc=1, device_id=(section, lax.rem(me + k + 1, n_dp)), device_id_type=MESH
        )

    def greet_section(k):
        pl.semaphore_signal(
            barrier, inc=1, device_id=(lax.rem(section + k + 1, n_section), me), device_id_type=MESH
        )

    repeat(n_dp - 1, greet_dp)
    repeat(n_section - 1, greet_section)
    load_theirs = pltpu.make_async_copy(grads.at[:, other], theirs, load_sem.at[0])
    load_mine = pltpu.make_async_copy(grads.at[:, core], mine, load_sem.at[1])
    load_theirs.start()
    load_mine.start()
    state_loads = [
        pltpu.make_async_copy(source, state.at[k], load_sem.at[2 + k])
        for k, source in enumerate((master, moment_one, moment_two))
    ]
    state_loads.append(pltpu.make_async_copy(bounds, bounds_in, load_sem.at[5]))
    for load in state_loads:
        load.start()

    pl.semaphore_wait(barrier, n_dp + n_section - 2)

    def pair_copy(off):
        z = lax.rem(chip + off, n_chip)
        return remote(
            theirs.at[z], paired.at[z], pair_send.at[off], pair_recv.at[off], section, partner
        )

    def order(k):
        return k + 1 if isinstance(k, int) and k + 1 < n_chip else lax.rem(k + 1, n_chip)

    load_theirs.wait()
    repeat(n_chip, lambda k: pair_copy(order(k)).start())
    load_mine.wait()

    def sum_copy(k):
        z = lax.rem(chip + k + 1, n_chip)
        return remote(
            outgoing.at[k], incoming.at[k], sum_send.at[k], sum_recv.at[k], section, z * PAIR + core
        )

    def send_sum(k):
        z = lax.rem(chip + k + 1, n_chip)
        pair_copy(k + 1).wait_recv()
        outgoing[k] = (mine[z] + paired[z]).astype(jnp.bfloat16)
        sum_copy(k).start()

    repeat(n_chip - 1, send_sum)
    pair_copy(0).wait_recv()
    mine[chip] = mine[chip] + paired[chip]

    def take_sum(k):
        sum_copy(k).wait_recv()
        mine[chip] = mine[chip] + incoming[k].astype(jnp.float32)

    repeat(n_chip - 1, take_sum)
    total_grad = mine[chip]

    for load in state_loads:
        load.wait()
    row_squares = jnp.sum(total_grad * total_grad, axis=1, keepdims=True)
    row = me * own_rows + lax.broadcasted_iota(jnp.int32, (own_rows, LANES), 0)
    lane = lax.broadcasted_iota(jnp.int32, (1, LANES), 1)
    low = jnp.zeros((1, LANES), jnp.int32)
    high = jnp.zeros((1, LANES), jnp.int32)
    for layer in range(layers):
        low = jnp.where(lane == layer, bounds_in[0, layer], low)
        high = jnp.where(lane == layer, bounds_in[0, layer + 1], high)
    inside = (row >= low) & (row < high)
    own_stats = jnp.sum(jnp.where(inside, row_squares, 0.0), axis=0, keepdims=True)
    good = (MICRO - skipped[0]).astype(jnp.float32)
    stats[place] = jnp.where(lane == layers, good, own_stats)

    def stat_copy(ahead, k):
        return remote(
            stats.at[place], stats.at[place],
            stat_send.at[ahead * n_dp + k], stat_recv.at[ahead * n_dp + k],
            lax.rem(section + ahead, n_section), lax.rem(me + k, n_dp),
        )

    def each_peer(act):
        for ahead in range(n_section - 1, 0, -1):
            repeat(n_dp, lambda k: act(stat_copy(ahead, k)))
        repeat(n_dp - 1, lambda k: act(stat_copy(0, k + 1)))

    each_peer(lambda copy: copy.start())
    step_value = jnp.full((1, 1), step[0], jnp.int32).astype(jnp.float32)
    fix_one = 1.0 - jnp.exp(step_value * math.log(beta_one))
    fix_two = 1.0 - jnp.exp(step_value * math.log(beta_two))
    layer_rows = jnp.where(lane < layers, high - low, 1).astype(jnp.float32)
    each_peer(lambda copy: copy.wait_recv())
    section_sum = jnp.sum(stats[pl.ds(section * n_dp, n_dp)], axis=0)
    everything = jnp.sum(stats[...], axis=0)
    total_good = jnp.sum(jnp.where(lane == layers, section_sum, 0.0), axis=1, keepdims=True)
    norms = jnp.sqrt(section_sum / (layer_rows * width)) / total_good
    norms_out[0] = norms
    total_sq = jnp.sum(jnp.where(lane < layers, everything, 0.0), axis=1, keepdims=True)
    grad_rms = jnp.sqrt(total_sq / (n_section * rows_all * width)) / total_good
    norms_out[1] = jnp.broadcast_to(grad_rms, (1, LANES))

    clipped = total_grad * (1.0 / (total_good * jnp.maximum(1.0, grad_rms)))
    one = beta_one * state[1] + (1.0 - beta_one) * clipped
    two = beta_two * state[2] + (1.0 - beta_two) * clipped * clipped
    update = one * (1.0 / fix_one) / (jnp.sqrt(two * (1.0 / fix_two)) + epsilon)
    master_new = state[0] - learn_rate * (update + weight_decay * state[0])
    params[me] = master_new.astype(jnp.bfloat16)

    def near_copy(off):
        block = lax.rem(chip + off, n_chip) * PAIR + core
        return remote(
            params.at[block], params.at[block], near_send.at[off], near_recv.at[off], section, partner
        )

    def row_copy(k):
        return remote(
            params.at[me], params.at[me], row_send.at[k], row_recv.at[k],
            section, lax.rem(chip + k + 1, n_chip) * PAIR + core,
        )

    repeat(n_chip - 1, lambda k: row_copy(k).start())
    near_copy(0).start()
    result[0] = master_new
    result[1] = one
    result[2] = two

    def pass_on(k):
        row_copy(k).wait_recv()
        near_copy(n_chip - 1 - k).start()

    repeat(n_chip - 1, pass_on)
    repeat(n_chip, lambda k: near_copy(k).wait_recv())
    repeat(n_chip, lambda k: pair_copy(k).wait_send())
    repeat(n_chip - 1, lambda k: sum_copy(k).wait_send())
    each_peer(lambda copy: copy.wait_send())
    repeat(n_chip - 1, lambda k: row_copy(k).wait_send())
    repeat(n_chip, lambda k: near_copy(k).wait_send())


def write_out(params, result, norms, params_out, master_next, first_next, second_next, layer_norms, grad_norm, sem):
    copies = [pltpu.make_async_copy(params, params_out, sem.at[3])]
    copies += [
        pltpu.make_async_copy(result.at[k], target, sem.at[k])
        for k, target in enumerate((master_next, first_next, second_next))
    ]
    for copy in copies:
        copy.start()
    layer_norms[...] = norms[0][:, : layer_norms.shape[1]]
    grad_norm[...] = norms[1][:, :1]
    for copy in copies:
        copy.wait()


def on_device(n_section, n_dp, grads, skipped, master, moment_one, moment_two, bounds, step):
    rows_all, width = grads.shape[2:]
    own_rows = master.shape[1]
    layers = bounds.shape[1] - 1
    n_chip = n_dp // PAIR
    smem = pl.BlockSpec(memory_space=pltpu.SMEM)
    hbm = pl.BlockSpec(memory_space=pltpu.HBM)
    held_bytes = rows_all * width * 2 + 3 * own_rows * width * 4 + SPARE
    vmem = pl.BlockSpec(memory_space=pltpu.VMEM)
    own = jax.ShapeDtypeStruct((own_rows, width), jnp.float32)
    dma = pltpu.SemaphoreType.DMA
    blocks = pltpu.VMEM((n_chip, own_rows, width), jnp.float32)
    halves = pltpu.VMEM((n_chip - 1, own_rows, width), jnp.bfloat16)
    held = pl.pallas_call(
        functools.partial(kernel, n_section, n_dp, layers),
        out_shape=(
            pltpu.VMEM((n_dp, own_rows, width), jnp.bfloat16),
            pltpu.VMEM((3, own_rows, width), jnp.float32),
            pltpu.VMEM((2, 1, LANES), jnp.float32),
        ),
        in_specs=[hbm, smem, hbm, hbm, hbm, hbm, smem],
        out_specs=(vmem, vmem, vmem),
        scratch_shapes=[
            blocks,
            blocks,
            blocks,
            halves,
            halves,
            pltpu.VMEM((n_section * n_dp, 1, LANES), jnp.float32),
            pltpu.VMEM((3, own_rows, width), jnp.float32),
            pltpu.SMEM(bounds.shape, jnp.int32),
            dma((6,)),
            dma((n_chip,)),
            dma((n_chip,)),
            dma((n_chip - 1,)),
            dma((n_chip - 1,)),
            dma((n_section * n_dp,)),
            dma((n_section * n_dp,)),
            dma((n_chip - 1,)),
            dma((n_chip - 1,)),
            dma((n_chip,)),
            dma((n_chip,)),
        ],
        compiler_params=pltpu.CompilerParams(
            collective_id=0, has_side_effects=True, vmem_limit_bytes=VMEM_BYTES - held_bytes
        ),
    )(
        grads.reshape(n_chip, PAIR, own_rows, width),
        skipped,
        master[0],
        moment_one[0],
        moment_two[0],
        bounds,
        step,
    )
    params, master_next, first_next, second_next, layer_norms, grad_norm = pl.pallas_call(
        write_out,
        out_shape=(
            jax.ShapeDtypeStruct((n_dp, own_rows, width), jnp.bfloat16),
            own,
            own,
            own,
            jax.ShapeDtypeStruct((1, layers), jnp.float32),
            jax.ShapeDtypeStruct((1, 1), jnp.float32),
        ),
        in_specs=[vmem] * 3,
        out_specs=(hbm, hbm, hbm, hbm, vmem, vmem),
        scratch_shapes=[dma((4,))],
        compiler_params=pltpu.CompilerParams(vmem_limit_bytes=SLACK),
    )(*held)
    return (
        params.reshape(1, rows_all, width),
        master_next[None],
        first_next[None],
        second_next[None],
        layer_norms,
        grad_norm.reshape(1),
    )


def solution(mesh):
    in_specs = (
        P("section", "dp", None, None),
        P("dp"),
        P("section", "dp", None),
        P("section", "dp", None),
        P("section", "dp", None),
        P("section", None),
        P(),
    )
    out_specs = (
        P("section", None, None),
        P("section", "dp", None),
        P("section", "dp", None),
        P("section", "dp", None),
        P("section", None),
        P(),
    )
    body = functools.partial(on_device, mesh.shape["section"], mesh.shape["dp"])
    return jax.shard_map(
        body, mesh=mesh, in_specs=in_specs, out_specs=out_specs, check_vma=False
    )
```

```python
import functools
import math

import jax
import jax.numpy as jnp
from jax import lax
from jax.experimental import pallas as pl
from jax.experimental.pallas import tpu as pltpu
from jax.sharding import PartitionSpec as P

MICRO = 32
PAIR = 2

beta_one = 0.9
beta_two = 0.95
learn_rate = 0.05
weight_decay = 0.1
epsilon = 1e-08

MESH = pl.DeviceIdType.MESH
LANES = 128
SLACK = 2**20
SPARE = 2**14
VMEM_BYTES = 67043328


def repeat(count, body):
    if count <= 8:
        for index in range(count):
            body(index)
    else:
        lax.fori_loop(0, count, lambda index, _: (body(index), None)[1], None)


def kernel(
    n_section,
    n_dp,
    layers,
    grads,
    skipped,
    master,
    moment_one,
    moment_two,
    bounds,
    step,
    params,
    result,
    norms_out,
    mine,
    theirs,
    paired,
    outgoing,
    incoming,
    stats,
    state,
    bounds_in,
    load_sem,
    pair_send,
    pair_recv,
    sum_send,
    sum_recv,
    stat_send,
    stat_recv,
    row_send,
    row_recv,
    near_send,
    near_recv,
):
    section = lax.axis_index("section")
    me = lax.axis_index("dp")
    n_chip = n_dp // PAIR
    chip, core = me // PAIR, lax.rem(me, PAIR)
    other = 1 - core
    partner = chip * PAIR + other
    own_rows, width = mine.shape[1], mine.shape[2]
    rows_all = n_dp * own_rows
    place = section * n_dp + me

    def remote(src, dst, send, recv, sec, dp):
        return pltpu.make_async_remote_copy(
            src_ref=src, dst_ref=dst, send_sem=send, recv_sem=recv,
            device_id=(sec, dp), device_id_type=MESH,
        )

    barrier = pltpu.get_barrier_semaphore()

    def sweep(body):
        if n_chip <= 8:
            middle = n_chip // 2 - 1
            for k in sorted(range(n_chip - 1), key=lambda k: k != middle):
                body(k)
        else:
            repeat(n_chip - 1, body)

    def greet_dp(k):
        pl.semaphore_signal(
            barrier, inc=1, device_id=(section, lax.rem(me + k + 1, n_dp)), device_id_type=MESH
        )

    def greet_section(k):
        pl.semaphore_signal(
            barrier, inc=1, device_id=(lax.rem(section + k + 1, n_section), me), device_id_type=MESH
        )

    repeat(n_dp - 1, greet_dp)
    repeat(n_section - 1, greet_section)
    load_theirs = pltpu.make_async_copy(grads.at[:, other], theirs, load_sem.at[0])
    load_mine = pltpu.make_async_copy(grads.at[:, core], mine, load_sem.at[1])
    load_theirs.start()
    load_mine.start()
    state_loads = [
        pltpu.make_async_copy(source, state.at[k], load_sem.at[2 + k])
        for k, source in enumerate((master, moment_one, moment_two))
    ]
    state_loads.append(pltpu.make_async_copy(bounds, bounds_in, load_sem.at[5]))
    for load in state_loads:
        load.start()

    pl.semaphore_wait(barrier, n_dp + n_section - 2)

    def pair_copy(off):
        z = lax.rem(chip + off, n_chip)
        return remote(
            theirs.at[z], paired.at[z], pair_send.at[off], pair_recv.at[off], section, partner
        )

    load_theirs.wait()
    sweep(lambda k: pair_copy(k + 1).start())
    pair_copy(0).start()
    load_mine.wait()

    def sum_copy(k):
        z = lax.rem(chip + k + 1, n_chip)
        return remote(
            outgoing.at[k], incoming.at[k], sum_send.at[k], sum_recv.at[k], section, z * PAIR + core
        )

    def send_sum(k):
        z = lax.rem(chip + k + 1, n_chip)
        pair_copy(k + 1).wait_recv()
        outgoing[k] = (mine[z] + paired[z]).astype(jnp.bfloat16)
        sum_copy(k).start()

    sweep(send_sum)
    pair_copy(0).wait_recv()
    mine[chip] = mine[chip] + paired[chip]

    def take_sum(k):
        sum_copy(k).wait_recv()
        mine[chip] = mine[chip] + incoming[k].astype(jnp.float32)

    sweep(take_sum)
    total_grad = mine[chip]

    for load in state_loads:
        load.wait()
    row_squares = jnp.sum(total_grad * total_grad, axis=1, keepdims=True)
    row = me * own_rows + lax.broadcasted_iota(jnp.int32, (own_rows, LANES), 0)
    lane = lax.broadcasted_iota(jnp.int32, (1, LANES), 1)
    low = jnp.zeros((1, LANES), jnp.int32)
    high = jnp.zeros((1, LANES), jnp.int32)
    for layer in range(layers):
        low = jnp.where(lane == layer, bounds_in[0, layer], low)
        high = jnp.where(lane == layer, bounds_in[0, layer + 1], high)
    inside = (row >= low) & (row < high)
    own_stats = jnp.sum(jnp.where(inside, row_squares, 0.0), axis=0, keepdims=True)
    good = (MICRO - skipped[0]).astype(jnp.float32)
    stats[place] = jnp.where(lane == layers, good, own_stats)

    def stat_copy(ahead, k):
        return remote(
            stats.at[place], stats.at[place],
            stat_send.at[ahead * n_dp + k], stat_recv.at[ahead * n_dp + k],
            lax.rem(section + ahead, n_section), lax.rem(me + k, n_dp),
        )

    def each_peer(act):
        for ahead in range(n_section - 1, 0, -1):
            repeat(n_dp, lambda k: act(stat_copy(ahead, k)))
        repeat(n_dp - 1, lambda k: act(stat_copy(0, k + 1)))

    each_peer(lambda copy: copy.start())
    step_value = jnp.full((1, 1), step[0], jnp.int32).astype(jnp.float32)
    fix_one = 1.0 - jnp.exp(step_value * math.log(beta_one))
    fix_two = 1.0 - jnp.exp(step_value * math.log(beta_two))
    layer_rows = jnp.where(lane < layers, high - low, 1).astype(jnp.float32)
    each_peer(lambda copy: copy.wait_recv())
    section_sum = jnp.sum(stats[pl.ds(section * n_dp, n_dp)], axis=0)
    everything = jnp.sum(stats[...], axis=0)
    total_good = jnp.sum(jnp.where(lane == layers, section_sum, 0.0), axis=1, keepdims=True)
    norms = jnp.sqrt(section_sum / (layer_rows * width)) / total_good
    norms_out[0] = norms
    total_sq = jnp.sum(jnp.where(lane < layers, everything, 0.0), axis=1, keepdims=True)
    grad_rms = jnp.sqrt(total_sq / (n_section * rows_all * width)) / total_good
    norms_out[1] = jnp.broadcast_to(grad_rms, (1, LANES))

    clipped = total_grad * (1.0 / (total_good * jnp.maximum(1.0, grad_rms)))
    one = beta_one * state[1] + (1.0 - beta_one) * clipped
    two = beta_two * state[2] + (1.0 - beta_two) * clipped * clipped
    update = one * (1.0 / fix_one) / (jnp.sqrt(two * (1.0 / fix_two)) + epsilon)
    master_new = state[0] - learn_rate * (update + weight_decay * state[0])
    params[me] = master_new.astype(jnp.bfloat16)

    def near_copy(off):
        block = lax.rem(chip + off, n_chip) * PAIR + core
        return remote(
            params.at[block], params.at[block], near_send.at[off], near_recv.at[off], section, partner
        )

    def row_copy(k):
        return remote(
            params.at[me], params.at[me], row_send.at[k], row_recv.at[k],
            section, lax.rem(chip + k + 1, n_chip) * PAIR + core,
        )

    sweep(lambda k: row_copy(k).start())
    near_copy(0).start()
    result[0] = master_new
    result[1] = one
    result[2] = two

    def pass_on(k):
        row_copy(k).wait_recv()
        near_copy(n_chip - 1 - k).start()

    repeat(n_chip, lambda k: pair_copy(k).wait_send())
    repeat(n_chip - 1, lambda k: sum_copy(k).wait_send())
    each_peer(lambda copy: copy.wait_send())
    sweep(pass_on)
    repeat(n_chip, lambda k: near_copy(k).wait_recv())
    repeat(n_chip - 1, lambda k: row_copy(k).wait_send())
    repeat(n_chip, lambda k: near_copy(k).wait_send())


def write_out(params, result, norms, params_out, master_next, first_next, second_next, layer_norms, grad_norm, sem):
    copies = [
        pltpu.make_async_copy(params.at[k], params_out.at[k], sem.at[3 + k])
        for k in range(params.shape[0])
    ]
    copies += [
        pltpu.make_async_copy(result.at[k], target, sem.at[k])
        for k, target in enumerate((master_next, first_next, second_next))
    ]
    for copy in copies:
        copy.start()
    layer_norms[...] = norms[0][:, : layer_norms.shape[1]]
    grad_norm[...] = norms[1][:, :1]
    for copy in copies:
        copy.wait()


def on_device(n_section, n_dp, grads, skipped, master, moment_one, moment_two, bounds, step):
    rows_all, width = grads.shape[2:]
    own_rows = master.shape[1]
    layers = bounds.shape[1] - 1
    n_chip = n_dp // PAIR
    smem = pl.BlockSpec(memory_space=pltpu.SMEM)
    hbm = pl.BlockSpec(memory_space=pltpu.HBM)
    held_bytes = rows_all * width * 2 + 3 * own_rows * width * 4 + SPARE
    vmem = pl.BlockSpec(memory_space=pltpu.VMEM)
    own = jax.ShapeDtypeStruct((own_rows, width), jnp.float32)
    dma = pltpu.SemaphoreType.DMA
    blocks = pltpu.VMEM((n_chip, own_rows, width), jnp.float32)
    halves = pltpu.VMEM((n_chip - 1, own_rows, width), jnp.bfloat16)
    held = pl.pallas_call(
        functools.partial(kernel, n_section, n_dp, layers),
        out_shape=(
            pltpu.VMEM((n_dp, own_rows, width), jnp.bfloat16),
            pltpu.VMEM((3, own_rows, width), jnp.float32),
            pltpu.VMEM((2, 1, LANES), jnp.float32),
        ),
        in_specs=[hbm, smem, hbm, hbm, hbm, hbm, smem],
        out_specs=(vmem, vmem, vmem),
        scratch_shapes=[
            blocks,
            blocks,
            blocks,
            halves,
            halves,
            pltpu.VMEM((n_section * n_dp, 1, LANES), jnp.float32),
            pltpu.VMEM((3, own_rows, width), jnp.float32),
            pltpu.SMEM(bounds.shape, jnp.int32),
            dma((6,)),
            dma((n_chip,)),
            dma((n_chip,)),
            dma((n_chip - 1,)),
            dma((n_chip - 1,)),
            dma((n_section * n_dp,)),
            dma((n_section * n_dp,)),
            dma((n_chip - 1,)),
            dma((n_chip - 1,)),
            dma((n_chip,)),
            dma((n_chip,)),
        ],
        compiler_params=pltpu.CompilerParams(
            collective_id=0, has_side_effects=True, vmem_limit_bytes=VMEM_BYTES - held_bytes
        ),
    )(
        grads.reshape(n_chip, PAIR, own_rows, width),
        skipped,
        master[0],
        moment_one[0],
        moment_two[0],
        bounds,
        step,
    )
    params, master_next, first_next, second_next, layer_norms, grad_norm = pl.pallas_call(
        write_out,
        out_shape=(
            jax.ShapeDtypeStruct((n_dp, own_rows, width), jnp.bfloat16),
            own,
            own,
            own,
            jax.ShapeDtypeStruct((1, layers), jnp.float32),
            jax.ShapeDtypeStruct((1, 1), jnp.float32),
        ),
        in_specs=[vmem] * 3,
        out_specs=(hbm, hbm, hbm, hbm, vmem, vmem),
        scratch_shapes=[dma((3 + n_dp,))],
        compiler_params=pltpu.CompilerParams(vmem_limit_bytes=SLACK),
    )(*held)
    return (
        params.reshape(1, rows_all, width),
        master_next[None],
        first_next[None],
        second_next[None],
        layer_norms,
        grad_norm.reshape(1),
    )


def solution(mesh):
    in_specs = (
        P("section", "dp", None, None),
        P("dp"),
        P("section", "dp", None),
        P("section", "dp", None),
        P("section", "dp", None),
        P("section", None),
        P(),
    )
    out_specs = (
        P("section", None, None),
        P("section", "dp", None),
        P("section", "dp", None),
        P("section", "dp", None),
        P("section", None),
        P(),
    )
    body = functools.partial(on_device, mesh.shape["section"], mesh.shape["dp"])
    return jax.shard_map(
        body, mesh=mesh, in_specs=in_specs, out_specs=out_specs, check_vma=False
    )
```
